32 devices in a mesh: worker: 8 (over y, x, core), mp: 4 (over z).
Axes of the slice: x: 2, y: 2, z: 4, core: 2. Of those that a mesh axis runs over, the one named last changes fastest.
Arguments:
- gradients: float32 [8, 2097152], P('worker', 'mp'), may hold values from -100 to 100
- neighbours: int32 [8, 3], replicated, may hold values from 0 to 7, as said below
- winner: int32 [1], replicated, may hold values from 0 to 7
Outputs:
- scores: float32 [8], replicated
- aggregate: float32 [2097152], P(('mp', 'worker'))
The draws below stay inside these ranges and needn't reach their ends.
Inputs may be any that keep to these rules, and one draw needn't show every extreme that they name: `neighbours`: row i lists 3 different workers, none of them equal to i.
All inputs are finite; a program needn't handle non-finite values.
Results may differ from the reference program's by a relative error of at most 0.0003.
Values may be sent and summed in bfloat16 or wider, within the bound.
A program may use at most 64 MiB of HBM per device.

```python
import math
import jax
import jax.numpy as jnp
from jax import lax

FAULTY = 3
WORKERS = 8
NBR = 3
PARAMS = 2097152


def draw_gradients(key, part):
    keys = jax.random.split(jax.random.fold_in(key, 11), 10)
    noise = jnp.clip(jax.random.normal(keys[0], (WORKERS, PARAMS), jnp.float32), -6.0, 6.0)
    position = jnp.arange(PARAMS, dtype=jnp.float32) / jnp.float32(PARAMS)
    scales = jnp.exp(jax.random.uniform(keys[1], (WORKERS, 1), jnp.float32, math.log(0.5), math.log(2.0)))
    column = 0.5 * jnp.exp(math.log(3.0) * position)[None, :]
    values = scales * column * noise
    loadings = jax.random.uniform(keys[8], (WORKERS, 4), jnp.float32, -1.0, 1.0)
    shared = jnp.clip(jax.random.normal(keys[9], (4, PARAMS), jnp.float32), -6.0, 6.0)
    for factor in range(4):
        values = values + column * loadings[:, factor:factor + 1] * shared[factor][None, :]
    ranking = jax.random.permutation(keys[4], WORKERS)
    faulty = (ranking < FAULTY).astype(jnp.float32)[:, None]
    sparse = (jax.random.uniform(keys[5], (WORKERS, PARAMS), jnp.float32) < 1.0 / 4096.0).astype(jnp.float32)
    size = jax.random.uniform(keys[6], (WORKERS, PARAMS), jnp.float32, 20.0, 40.0)
    sign = jnp.where(jax.random.uniform(keys[7], (WORKERS, PARAMS), jnp.float32) < 0.5, -1.0, 1.0)
    values = values + faulty * sparse * sign * size * column
    return jnp.clip(values, -100.0, 100.0).astype(jnp.float32)


def draw_neighbours(key, part):
    keys = jax.random.split(jax.random.fold_in(key, 23), WORKERS)
    orders = jax.vmap(lambda single: jax.random.permutation(single, WORKERS - 1))(keys)[:, :NBR]
    orders = orders.astype(jnp.int32)
    own_index = jnp.arange(WORKERS, dtype=jnp.int32)[:, None]
    return (orders + (orders >= own_index).astype(jnp.int32)).astype(jnp.int32)


def setup_inputs(seed: int = 0) -> dict:
    streams_of = jax.random.split(jax.random.key(seed), 4)
    return {
        "gradients": draw_gradients(jax.random.fold_in(streams_of[3], 71), 0),
        "neighbours": draw_neighbours(jax.random.fold_in(streams_of[3], 71), 0),
        "winner": jax.random.randint(streams_of[2], (1,), 0, WORKERS).astype(jnp.int32),
    }


def reference(gradients, neighbours, winner):
    rounded = gradients.astype(jnp.bfloat16)
    gram_matrix = jnp.dot(rounded, rounded.T, preferred_element_type=jnp.float32)
    squares = jnp.diagonal(gram_matrix)
    distance = squares[:, None] + squares[None, :] - 2.0 * gram_matrix
    chosen = jnp.take_along_axis(distance, neighbours, axis=1)
    scores = jnp.sum(chosen, axis=1) / jnp.float32(NBR * PARAMS)
    aggregate = lax.dynamic_index_in_dim(gradients, winner[0], 0, keepdims=False)
    return (scores, aggregate)
```

```python
import functools

import jax
import jax.numpy as jnp
from jax import lax
from jax.experimental import pallas as pl
from jax.experimental.pallas import tpu as pltpu
from jax.sharding import PartitionSpec as P

MESH = pl.DeviceIdType.MESH
LANES = 128
CHUNKS = 4


def flip(index, offset, size):
    result, bit = 0, 1
    while bit < size:
        digit = (index // bit) % 2
        if (offset // bit) % 2:
            digit = 1 - digit
        result = result + digit * bit
        bit *= 2
    return result


def kernel(
    workers,
    planes,
    total_entries,
    nb_ref,
    win_ref,
    g_ref,
    scores_ref,
    out_ref,
    stage,
    rounded,
    recv,
    rest,
    rest_in,
    rest_recv,
    dist,
    part,
    zbuf,
    plane_part,
    pbuf,
    load_sem,
    gsend,
    grecv,
    osend,
    orecv,
    rsend,
    rrecv,
    zsend,
    zrecv,
    psend,
    precv,
):
    me = lax.axis_index("worker")
    plane = lax.axis_index("mp")
    core = me % 2
    chip = me // 2
    chips = workers // 2
    rows = stage.shape[1]
    span = rows // CHUNKS
    order = sorted(range(2, workers), key=lambda o: (bin(o // 2).count("1"), o % 2, o)) + [1, 0]
    near = [o for o in range(1, workers) if bin(o // 2).count("1") < 2]
    far = [o for o in order if bin(o // 2).count("1") >= 2]
    peer = [flip(me, o, workers) for o in range(workers)]

    barrier = pltpu.get_barrier_semaphore()
    for o in range(1, workers):
        pl.semaphore_signal(barrier, inc=1, device_id={"worker": peer[o]}, device_id_type=MESH)
    for z in range(1, planes):
        pl.semaphore_signal(
            barrier, inc=1, device_id={"mp": (plane + z) % planes}, device_id_type=MESH
        )

    def load(o):
        first = pl.multiple_of(peer[o] * rows, rows)
        return pltpu.make_async_copy(g_ref.at[pl.ds(first, rows), :], stage.at[o], load_sem.at[o])

    for o in order:
        load(o).start()

    def gram_copy(o, c, slot):
        at = pl.ds(c * span, span)
        return pltpu.make_async_remote_copy(
            src_ref=rounded.at[o, at, :],
            dst_ref=recv.at[slot, at, :],
            send_sem=gsend.at[o, c],
            recv_sem=grecv.at[o, c],
            device_id={"worker": peer[o]},
            device_id_type=MESH,
        )

    def whole_copy(o, slot):
        return pltpu.make_async_remote_copy(
            src_ref=rounded.at[o],
            dst_ref=recv.at[slot],
            send_sem=gsend.at[o, 0],
            recv_sem=grecv.at[o, 0],
            device_id={"worker": peer[o]},
            device_id_type=MESH,
        )

    keep = jnp.where(win_ref[0] == me, 1.0, 0.0).astype(jnp.float32)
    block = 128

    def convert(o):
        parity = peer[o] % 2
        where = peer[o] // 2

        def one(step, carry):
            at = pl.ds(pl.multiple_of(step * block, block), block)
            x = stage[o, at, :]
            hi = x.astype(jnp.bfloat16)
            if o == 0:
                recv[me, at, :] = hi
            else:
                rounded[o, at, :] = hi
            rest[parity, where, at, :] = ((x - hi.astype(jnp.float32)) * keep).astype(jnp.bfloat16)
            return carry

        lax.fori_loop(0, rows // block, one, 0)

    for n, o in enumerate(order):
        load(o).wait()
        convert(o)
        if n == 0:
            pl.semaphore_wait(barrier, workers - 1 + planes - 1)
        if o in near:
            whole_copy(o, me).start()
        elif o in far and o % 2 == 1:
            for c in range(CHUNKS):
                gram_copy(o - 1, c, me).start()
                gram_copy(o, c, me).start()

    swap = pltpu.make_async_remote_copy(
        src_ref=rest.at[1 - core],
        dst_ref=rest_in,
        send_sem=osend,
        recv_sem=orecv,
        device_id={"worker": peer[1]},
        device_id_type=MESH,
    )
    swap.start()
    swap.wait_recv()

    def combine(step, carry):
        at = pl.ds(pl.multiple_of(step * block, block), block)
        for q in range(chips):
            rest_in[q, at, :] = rest_in[q, at, :] + rest[core, q, at, :]
        return carry

    lax.fori_loop(0, rows // block, combine, 0)

    def rest_copy(ox):
        return pltpu.make_async_remote_copy(
            src_ref=rest_in.at[flip(chip, ox, chips)],
            dst_ref=rest_recv.at[ox],
            send_sem=rsend.at[ox],
            recv_sem=rrecv.at[ox],
            device_id={"worker": peer[2 * ox]},
            device_id_type=MESH,
        )

    rest_order = sorted(range(1, chips), key=lambda ox: bin(ox).count("1"))

    pairs = [(i, k) for i in range(workers) for k in range(i, workers)]

    def gram(first, accs):
        def one(step, accs):
            at = pl.ds(pl.multiple_of(first + step * 16, 16), 16)
            xs = [recv[i, at, :].astype(jnp.float32) for i in range(workers)]
            lo = [x[:8] for x in xs]
            hi = [x[8:] for x in xs]
            return tuple(
                a + (lo[i] * lo[k] + hi[i] * hi[k]) for a, (i, k) in zip(accs, pairs)
            )

        return lax.fori_loop(0, span // 16, one, accs)

    accs = tuple(jnp.zeros((8, LANES), jnp.float32) for _ in pairs)
    for o in near:
        whole_copy(o, peer[o]).wait_recv()
    for c in range(CHUNKS):
        if c == CHUNKS - 1:
            for ox in rest_order:
                rest_copy(ox).start()
        for o in far:
            gram_copy(o, c, peer[o]).wait_recv()
        accs = gram(c * span, accs)

    value = dict(zip(pairs, accs))
    for i, k in pairs:
        if i == k:
            dist[i * workers + i] = jnp.zeros((8, LANES), jnp.float32)
        else:
            d = value[i, i] + value[k, k] - 2.0 * value[i, k]
            dist[i * workers + k] = d
            dist[k * workers + i] = d
    for i in range(workers):
        s = dist[i * workers + nb_ref[i, 0]]
        for j in range(1, nb_ref.shape[1]):
            s = s + dist[i * workers + nb_ref[i, j]]
        part[pl.ds(i, 1), :] = jnp.sum(s, axis=0, keepdims=True)

    def z_copy(z):
        return pltpu.make_async_remote_copy(
            src_ref=part,
            dst_ref=zbuf.at[z],
            send_sem=zsend.at[z],
            recv_sem=zrecv.at[z],
            device_id={"mp": (plane + z) % planes},
            device_id_type=MESH,
        )

    def p_copy(o):
        return pltpu.make_async_remote_copy(
            src_ref=plane_part,
            dst_ref=pbuf.at[o],
            send_sem=psend.at[o],
            recv_sem=precv.at[o],
            device_id={"worker": peer[o]},
            device_id_type=MESH,
        )

    for z in range(1, planes):
        z_copy(z).start()
    total = part[...]
    for z in range(1, planes):
        z_copy(z).wait_recv()
        total = total + zbuf[z]
    plane_part[...] = total
    for o in range(1, workers):
        p_copy(o).start()

    for ox in rest_order:
        rest_copy(ox).wait_recv()

    def finish(step, carry):
        at = pl.ds(pl.multiple_of(step * block, block), block)
        low = rest_in[chip, at, :].astype(jnp.float32)
        for ox in rest_order:
            low = low + rest_recv[ox, at, :].astype(jnp.float32)
        out_ref[at, :] = recv[win_ref[0], at, :].astype(jnp.float32) + low
        return carry

    lax.fori_loop(0, rows // block, finish, 0)

    for o in range(1, workers):
        p_copy(o).wait_recv()
        total = total + pbuf[o]
    column = jnp.sum(total, axis=1, keepdims=True) / jnp.float32(total_entries)
    line = lax.broadcasted_iota(jnp.int32, (workers, LANES), 0)
    lane = lax.broadcasted_iota(jnp.int32, (workers, LANES), 1)
    scores_ref[...] = jnp.sum(
        jnp.where(line == lane, column, 0.0), axis=0, keepdims=True
    )[:, :workers]

    swap.wait_send()
    for o in near:
        whole_copy(o, me).wait_send()
    for o in far:
        for c in range(CHUNKS):
            gram_copy(o, c, me).wait_send()
    for ox in rest_order:
        rest_copy(ox).wait_send()
    for z in range(1, planes):
        z_copy(z).wait_send()
    for o in range(1, workers):
        p_copy(o).wait_send()


def solution(mesh):
    workers = mesh.shape["worker"]
    planes = mesh.shape["mp"]
    chips = workers // 2

    def body(gradients, neighbours, winner):
        length = gradients.shape[1]
        rows = length // (LANES * workers)
        entries = neighbours.shape[1] * length * planes
        bf16, f32 = jnp.bfloat16, jnp.float32
        dma = pltpu.SemaphoreType.DMA
        scores, aggregate = pl.pallas_call(
            functools.partial(kernel, workers, planes, entries),
            out_shape=(
                jax.ShapeDtypeStruct((1, workers), f32),
                jax.ShapeDtypeStruct((rows, LANES), f32),
            ),
            in_specs=[
                pl.BlockSpec(memory_space=pltpu.SMEM),
                pl.BlockSpec(memory_space=pltpu.SMEM),
                pl.BlockSpec(memory_space=pl.ANY),
            ],
            out_specs=(
                pl.BlockSpec(memory_space=pltpu.VMEM),
                pl.BlockSpec(memory_space=pltpu.VMEM),
            ),
            scratch_shapes=[
                pltpu.VMEM((workers, rows, LANES), f32),
                pltpu.VMEM((workers, rows, LANES), bf16),
                pltpu.VMEM((workers, rows, LANES), bf16),
                pltpu.VMEM((2, chips, rows, LANES), bf16),
                pltpu.VMEM((chips, rows, LANES), bf16),
                pltpu.VMEM((chips, rows, LANES), bf16),
                pltpu.VMEM((workers * workers, 8, LANES), f32),
                pltpu.VMEM((workers, LANES), f32),
                pltpu.VMEM((planes, workers, LANES), f32),
                pltpu.VMEM((workers, LANES), f32),
                pltpu.VMEM((workers, workers, LANES), f32),
                dma((workers,)),
                dma((workers, CHUNKS)),
                dma((workers, CHUNKS)),
                dma,
                dma,
                dma((chips,)),
                dma((chips,)),
                dma((planes,)),
                dma((planes,)),
                dma((workers,)),
                dma((workers,)),
            ],
            compiler_params=pltpu.CompilerParams(collective_id=0, has_side_effects=True),
        )(neighbours, winner, gradients.reshape(length // LANES, LANES))
        return scores.reshape(workers), aggregate.reshape(rows * LANES)

    in_specs = (P("worker", "mp"), P(), P())
    out_specs = (P(), P(("mp", "worker")))
    return jax.shard_map(body, mesh=mesh, in_specs=in_specs, out_specs=out_specs, check_vma=False)
```

```python
import functools

import jax
import jax.numpy as jnp
from jax import lax
from jax.experimental import pallas as pl
from jax.experimental.pallas import tpu as pltpu
from jax.sharding import PartitionSpec as P

MESH = pl.DeviceIdType.MESH
LANES = 128
CHUNKS = 4


def flip(index, offset, size):
    result, bit = 0, 1
    while bit < size:
        digit = (index // bit) % 2
        if (offset // bit) % 2:
            digit = 1 - digit
        result = result + digit * bit
        bit *= 2
    return result


def kernel(
    workers,
    planes,
    total_entries,
    nb_hbm,
    win_ref,
    g_ref,
    scores_ref,
    out_ref,
    nb_ref,
    stage,
    rounded,
    recv,
    rest,
    rest_in,
    rest_recv,
    relay,
    dist,
    part,
    zbuf,
    plane_part,
    pbuf,
    small_sem,
    load_sem,
    gsend,
    grecv,
    osend,
    orecv,
    ysend,
    yrecv,
    rsend,
    rrecv,
    zsend,
    zrecv,
    psend,
    precv,
):
    me = lax.axis_index("worker")
    plane = lax.axis_index("mp")
    core = me % 2
    chip = me // 2
    chips = workers // 2
    rows = stage.shape[1]
    span = rows // CHUNKS
    order = sorted(range(2, workers), key=lambda o: (bin(o // 2).count("1"), o % 2, o)) + [1, 0]
    near = [o for o in range(1, workers) if bin(o // 2).count("1") < 2]
    far = [o for o in order if bin(o // 2).count("1") >= 2]
    peer = [flip(me, o, workers) for o in range(workers)]

    barrier = pltpu.get_barrier_semaphore()
    for o in range(1, workers):
        pl.semaphore_signal(barrier, inc=1, device_id={"worker": peer[o]}, device_id_type=MESH)
    for z in range(1, planes):
        pl.semaphore_signal(
            barrier, inc=1, device_id={"mp": (plane + z) % planes}, device_id_type=MESH
        )

    def load(o):
        first = pl.multiple_of(peer[o] * rows, rows)
        return pltpu.make_async_copy(g_ref.at[pl.ds(first, rows), :], stage.at[o], load_sem.at[o])

    lists = pltpu.make_async_copy(nb_hbm, nb_ref, small_sem)
    load(order[0]).start()
    lists.start()
    for o in order[1:]:
        load(o).start()

    def gram_copy(o, c, slot):
        at = pl.ds(c * span, span)
        return pltpu.make_async_remote_copy(
            src_ref=rounded.at[o, at, :],
            dst_ref=recv.at[slot, at, :],
            send_sem=gsend.at[o, c],
            recv_sem=grecv.at[o, c],
            device_id={"worker": peer[o]},
            device_id_type=MESH,
        )

    def whole_copy(o, slot):
        return pltpu.make_async_remote_copy(
            src_ref=rounded.at[o],
            dst_ref=recv.at[slot],
            send_sem=gsend.at[o, 0],
            recv_sem=grecv.at[o, 0],
            device_id={"worker": peer[o]},
            device_id_type=MESH,
        )

    keep = jnp.where(win_ref[0] == me, 1.0, 0.0).astype(jnp.float32)
    block = 128

    def convert(o):
        parity = peer[o] % 2
        where = peer[o] // 2

        def one(step, carry):
            at = pl.ds(pl.multiple_of(step * block, block), block)
            x = stage[o, at, :]
            hi = x.astype(jnp.bfloat16)
            if o == 0:
                recv[me, at, :] = hi
            else:
                rounded[o, at, :] = hi
            rest[parity, where, at, :] = ((x - hi.astype(jnp.float32)) * keep).astype(jnp.bfloat16)
            return carry

        lax.fori_loop(0, rows // block, one, 0)

    def swap(ox):
        there = flip(chip, ox, chips)
        return pltpu.make_async_remote_copy(
            src_ref=rest.at[1 - core, there],
            dst_ref=rest_in.at[there],
            send_sem=osend.at[ox],
            recv_sem=orecv.at[ox],
            device_id={"worker": peer[1]},
            device_id_type=MESH,
        )

    def add_to_rest(there, first, count, other):
        def one(step, carry):
            at = pl.ds(pl.multiple_of(first + step * block, block), block)
            rest_in[there, at, :] = rest_in[there, at, :] + other(at)
            return carry

        lax.fori_loop(0, count // block, one, 0)

    def combine(ox):
        there = flip(chip, ox, chips)
        swap(ox).wait_recv()
        add_to_rest(there, 0, rows, lambda at: rest[core, there, at, :])

    split = chips == 4
    half = rows // 2

    def relay_copy(ox):
        return pltpu.make_async_remote_copy(
            src_ref=rest_in.at[flip(chip, 3, chips), pl.ds((ox - 1) * half, half), :],
            dst_ref=relay.at[ox - 1],
            send_sem=ysend.at[ox - 1],
            recv_sem=yrecv.at[ox - 1],
            device_id={"worker": peer[2 * ox]},
            device_id_type=MESH,
        )

    for n, o in enumerate(order):
        load(o).wait()
        convert(o)
        if n == 0:
            pl.semaphore_wait(barrier, workers - 1 + planes - 1)
        if o in near:
            whole_copy(o, me).start()
        if o % 2 == 1:
            swap(o // 2).start()

    if split:
        combine(3)
        relay_copy(1).start()
        relay_copy(2).start()
    for o in far[::2]:
        for c in range(CHUNKS):
            gram_copy(o, c, me).start()
            gram_copy(o + 1, c, me).start()
    for ox in range(chips):
        if not (split and ox == 3):
            combine(ox)

    def rest_copy(ox):
        return pltpu.make_async_remote_copy(
            src_ref=rest_in.at[flip(chip, ox, chips)],
            dst_ref=rest_recv.at[ox],
            send_sem=rsend.at[ox],
            recv_sem=rrecv.at[ox],
            device_id={"worker": peer[2 * ox]},
            device_id_type=MESH,
        )

    rest_order = sorted(range(1, chips), key=lambda ox: bin(ox).count("1"))
    if split:
        rest_order = [1, 2]

    pairs = [(i, k) for i in range(workers) for k in range(i, workers)]

    def gram(first, accs):
        def one(step, accs):
            at = pl.ds(pl.multiple_of(first + step * 16, 16), 16)
            xs = [recv[i, at, :].astype(jnp.float32) for i in range(workers)]
            lo = [x[:8] for x in xs]
            hi = [x[8:] for x in xs]
            return tuple(
                a + (lo[i] * lo[k] + hi[i] * hi[k]) for a, (i, k) in zip(accs, pairs)
            )

        return lax.fori_loop(0, span // 16, one, accs)

    accs = tuple(jnp.zeros((8, LANES), jnp.float32) for _ in pairs)
    for o in near:
        whole_copy(o, peer[o]).wait_recv()
    for c in range(CHUNKS):
        if c == CHUNKS - 2:
            for ox in rest_order:
                if split:
                    first = (ox - 1) * half
                    relay_copy(ox).wait_recv()
                    add_to_rest(
                        flip(chip, 3 - ox, chips),
                        first,
                        half,
                        lambda at, first=first, ox=ox: relay[
                            ox - 1, pl.ds(pl.multiple_of(at.start - first, block), block), :
                        ],
                    )
            for ox in rest_order:
                rest_copy(ox).start()
        for o in far:
            gram_copy(o, c, peer[o]).wait_recv()
        accs = gram(c * span, accs)

    value = dict(zip(pairs, accs))
    for i, k in pairs:
        if i == k:
            dist[i * workers + i] = jnp.zeros((8, LANES), jnp.float32)
        else:
            d = value[i, i] + value[k, k] - 2.0 * value[i, k]
            dist[i * workers + k] = d
            dist[k * workers + i] = d
    lists.wait()
    for i in range(workers):
        s = dist[i * workers + nb_ref[0, i]]
        for j in range(1, nb_ref.shape[0]):
            s = s + dist[i * workers + nb_ref[j, i]]
        part[pl.ds(i, 1), :] = jnp.sum(s, axis=0, keepdims=True)

    def z_copy(z):
        return pltpu.make_async_remote_copy(
            src_ref=part,
            dst_ref=zbuf.at[z],
            send_sem=zsend.at[z],
            recv_sem=zrecv.at[z],
            device_id={"mp": (plane + z) % planes},
            device_id_type=MESH,
        )

    def p_copy(o):
        return pltpu.make_async_remote_copy(
            src_ref=plane_part,
            dst_ref=pbuf.at[o],
            send_sem=psend.at[o],
            recv_sem=precv.at[o],
            device_id={"worker": peer[o]},
            device_id_type=MESH,
        )

    for z in range(1, planes):
        z_copy(z).start()
    total = part[...]
    for z in range(1, planes):
        z_copy(z).wait_recv()
        total = total + zbuf[z]
    plane_part[...] = total
    for o in range(1, workers):
        p_copy(o).start()

    for ox in rest_order:
        rest_copy(ox).wait_recv()

    def finish(step, carry):
        at = pl.ds(pl.multiple_of(step * block, block), block)
        low = rest_in[chip, at, :].astype(jnp.float32)
        for ox in rest_order:
            low = low + rest_recv[ox, at, :].astype(jnp.float32)
        out_ref[at, :] = recv[win_ref[0], at, :].astype(jnp.float32) + low
        return carry

    lax.fori_loop(0, rows // block, finish, 0)

    for o in range(1, workers):
        p_copy(o).wait_recv()
        total = total + pbuf[o]
    column = jnp.sum(total, axis=1, keepdims=True) / jnp.float32(total_entries)
    line = lax.broadcasted_iota(jnp.int32, (workers, LANES), 0)
    lane = lax.broadcasted_iota(jnp.int32, (workers, LANES), 1)
    scores_ref[...] = jnp.sum(
        jnp.where(line == lane, column, 0.0), axis=0, keepdims=True
    )[:, :workers]

    for ox in range(chips):
        swap(ox).wait_send()
    if split:
        relay_copy(1).wait_send()
        relay_copy(2).wait_send()
    for o in near:
        whole_copy(o, me).wait_send()
    for o in far:
        for c in range(CHUNKS):
            gram_copy(o, c, me).wait_send()
    for ox in rest_order:
        rest_copy(ox).wait_send()
    for z in range(1, planes):
        z_copy(z).wait_send()
    for o in range(1, workers):
        p_copy(o).wait_send()


def emit(scores_ref, block_ref, scores_out, block_out, sems):
    copies = [
        pltpu.make_async_copy(block_ref, block_out, sems.at[0]),
        pltpu.make_async_copy(scores_ref, scores_out, sems.at[1]),
    ]
    for copy in copies:
        copy.start()
    for copy in copies:
        copy.wait()


def solution(mesh):
    workers = mesh.shape["worker"]
    planes = mesh.shape["mp"]
    chips = workers // 2

    def body(gradients, neighbours, winner):
        length = gradients.shape[1]
        rows = length // (LANES * workers)
        entries = neighbours.shape[1] * length * planes
        bf16, f32 = jnp.bfloat16, jnp.float32
        dma = pltpu.SemaphoreType.DMA
        scores, aggregate = pl.pallas_call(
            functools.partial(kernel, workers, planes, entries),
            out_shape=(
                pltpu.VMEM((1, workers), f32),
                pltpu.VMEM((rows, LANES), f32),
            ),
            in_specs=[
                pl.BlockSpec(memory_space=pltpu.HBM),
                pl.BlockSpec(memory_space=pltpu.SMEM),
                pl.BlockSpec(memory_space=pltpu.HBM),
            ],
            out_specs=(
                pl.BlockSpec(memory_space=pltpu.VMEM),
                pl.BlockSpec(memory_space=pltpu.VMEM),
            ),
            scratch_shapes=[
                pltpu.SMEM(neighbours.shape[::-1], jnp.int32),
                pltpu.VMEM((workers, rows, LANES), f32),
                pltpu.VMEM((workers, rows, LANES), bf16),
                pltpu.VMEM((workers, rows, LANES), bf16),
                pltpu.VMEM((2, chips, rows, LANES), bf16),
                pltpu.VMEM((chips, rows, LANES), bf16),
                pltpu.VMEM((chips, rows, LANES), bf16),
                pltpu.VMEM((2, rows // 2, LANES), bf16),
                pltpu.VMEM((workers * workers, 8, LANES), f32),
                pltpu.VMEM((workers, LANES), f32),
                pltpu.VMEM((planes, workers, LANES), f32),
                pltpu.VMEM((workers, LANES), f32),
                pltpu.VMEM((workers, workers, LANES), f32),
                dma,
                dma((workers,)),
                dma((workers, CHUNKS)),
                dma((workers, CHUNKS)),
                dma((chips,)),
                dma((chips,)),
                dma((2,)),
                dma((2,)),
                dma((chips,)),
                dma((chips,)),
                dma((planes,)),
                dma((planes,)),
                dma((workers,)),
                dma((workers,)),
            ],
            compiler_params=pltpu.CompilerParams(
                collective_id=0, has_side_effects=True, vmem_limit_bytes=63_500_000
            ),
        )(neighbours.T, winner, gradients.reshape(length // LANES, LANES))
        scores, aggregate = pl.pallas_call(
            emit,
            out_shape=(
                jax.ShapeDtypeStruct(scores.shape, f32),
                jax.ShapeDtypeStruct(aggregate.shape, f32),
            ),
            in_specs=[pl.BlockSpec(memory_space=pltpu.VMEM)] * 2,
            out_specs=(pl.BlockSpec(memory_space=pl.ANY),) * 2,
            scratch_shapes=[dma((2,))],
            compiler_params=pltpu.CompilerParams(vmem_limit_bytes=8 * 1024 * 1024),
        )(scores, aggregate)
        return scores.reshape(workers), aggregate.reshape(rows * LANES)

    in_specs = (P("worker", "mp"), P(), P())
    out_specs = (P(), P(("mp", "worker")))
    return jax.shard_map(body, mesh=mesh, in_specs=in_specs, out_specs=out_specs, check_vma=False)
```

```python
import functools

import jax
import jax.numpy as jnp
from jax import lax
from jax.experimental import pallas as pl
from jax.experimental.pallas import tpu as pltpu
from jax.sharding import PartitionSpec as P

MESH = pl.DeviceIdType.MESH
LANES = 128
CHUNKS = 4


def flip(index, offset, size):
    result, bit = 0, 1
    while bit < size:
        digit = (index // bit) % 2
        if (offset // bit) % 2:
            digit = 1 - digit
        result = result + digit * bit
        bit *= 2
    return result


def kernel(
    workers,
    planes,
    total_entries,
    nb_hbm,
    win_ref,
    g_ref,
    scores_ref,
    out_ref,
    nb_ref,
    stage,
    rounded,
    recv,
    rest,
    rest_in,
    rest_recv,
    relay,
    dist,
    part,
    zbuf,
    plane_part,
    pbuf,
    small_sem,
    load_sem,
    gsend,
    grecv,
    osend,
    orecv,
    ysend,
    yrecv,
    rsend,
    rrecv,
    zsend,
    zrecv,
    psend,
    precv,
):
    me = lax.axis_index("worker")
    plane = lax.axis_index("mp")
    core = me % 2
    chip = me // 2
    chips = workers // 2
    rows = stage.shape[1]
    span = rows // CHUNKS
    order = sorted(range(2, workers), key=lambda o: (bin(o // 2).count("1"), o % 2, o)) + [1, 0]
    near = [o for o in range(1, workers) if bin(o // 2).count("1") < 2]
    far = [o for o in order if bin(o // 2).count("1") >= 2]
    peer = [flip(me, o, workers) for o in range(workers)]

    barrier = pltpu.get_barrier_semaphore()
    for o in range(1, workers):
        pl.semaphore_signal(barrier, inc=1, device_id={"worker": peer[o]}, device_id_type=MESH)
    for z in range(1, planes):
        pl.semaphore_signal(
            barrier, inc=1, device_id={"mp": (plane + z) % planes}, device_id_type=MESH
        )

    def load(o):
        first = pl.multiple_of(peer[o] * rows, rows)
        return pltpu.make_async_copy(g_ref.at[pl.ds(first, rows), :], stage.at[o], load_sem.at[o])

    lists = pltpu.make_async_copy(nb_hbm, nb_ref, small_sem)
    load(order[0]).start()
    lists.start()
    for o in order[1:]:
        load(o).start()

    def gram_copy(o, c, slot):
        at = pl.ds(c * span, span)
        return pltpu.make_async_remote_copy(
            src_ref=rounded.at[o, at, :],
            dst_ref=recv.at[slot, at, :],
            send_sem=gsend.at[o, c],
            recv_sem=grecv.at[o, c],
            device_id={"worker": peer[o]},
            device_id_type=MESH,
        )

    def whole_copy(o, slot):
        return pltpu.make_async_remote_copy(
            src_ref=rounded.at[o],
            dst_ref=recv.at[slot],
            send_sem=gsend.at[o, 0],
            recv_sem=grecv.at[o, 0],
            device_id={"worker": peer[o]},
            device_id_type=MESH,
        )

    keep = jnp.where(win_ref[0] == me, 1.0, 0.0).astype(jnp.float32)
    block = 128

    def convert(o):
        parity = peer[o] % 2
        where = peer[o] // 2

        def one(step, carry):
            at = pl.ds(pl.multiple_of(step * block, block), block)
            x = stage[o, at, :]
            hi = x.astype(jnp.bfloat16)
            if o == 0:
                recv[me, at, :] = hi
            else:
                rounded[o, at, :] = hi
            rest[parity, where, at, :] = ((x - hi.astype(jnp.float32)) * keep).astype(jnp.bfloat16)
            return carry

        lax.fori_loop(0, rows // block, one, 0)

    def swap(ox):
        there = flip(chip, ox, chips)
        return pltpu.make_async_remote_copy(
            src_ref=rest.at[1 - core, there],
            dst_ref=rest_in.at[there],
            send_sem=osend.at[ox],
            recv_sem=orecv.at[ox],
            device_id={"worker": peer[1]},
            device_id_type=MESH,
        )

    def add_to_rest(there, first, count, other):
        def one(step, carry):
            at = pl.ds(pl.multiple_of(first + step * block, block), block)
            rest_in[there, at, :] = rest_in[there, at, :] + other(at)
            return carry

        lax.fori_loop(0, count // block, one, 0)

    def combine(ox):
        there = flip(chip, ox, chips)
        swap(ox).wait_recv()
        add_to_rest(there, 0, rows, lambda at: rest[core, there, at, :])

    split = chips == 4
    half = rows // 2

    def relay_copy(ox):
        return pltpu.make_async_remote_copy(
            src_ref=rest_in.at[flip(chip, 3, chips), pl.ds((ox - 1) * half, half), :],
            dst_ref=relay.at[ox - 1],
            send_sem=ysend.at[ox - 1],
            recv_sem=yrecv.at[ox - 1],
            device_id={"worker": peer[2 * ox]},
            device_id_type=MESH,
        )

    for n, o in enumerate(order):
        load(o).wait()
        convert(o)
        if n == 0:
            pl.semaphore_wait(barrier, workers - 1 + planes - 1)
        if o in near:
            whole_copy(o, me).start()
        if o % 2 == 1:
            swap(o // 2).start()

    for o in far[::2]:
        for c in range(CHUNKS):
            gram_copy(o, c, me).start()
            gram_copy(o + 1, c, me).start()
    if split:
        combine(3)
        relay_copy(1).start()
        relay_copy(2).start()
    for ox in range(chips):
        if not (split and ox == 3):
            combine(ox)

    def rest_copy(ox):
        return pltpu.make_async_remote_copy(
            src_ref=rest_in.at[flip(chip, ox, chips)],
            dst_ref=rest_recv.at[ox],
            send_sem=rsend.at[ox],
            recv_sem=rrecv.at[ox],
            device_id={"worker": peer[2 * ox]},
            device_id_type=MESH,
        )

    rest_order = sorted(range(1, chips), key=lambda ox: bin(ox).count("1"))
    if split:
        rest_order = [1, 2]

    pairs = [(i, k) for i in range(workers) for k in range(i, workers)]

    def gram(first, accs):
        def one(step, accs):
            at = pl.ds(pl.multiple_of(first + step * 16, 16), 16)
            xs = [recv[i, at, :].astype(jnp.float32) for i in range(workers)]
            lo = [x[:8] for x in xs]
            hi = [x[8:] for x in xs]
            return tuple(
                a + (lo[i] * lo[k] + hi[i] * hi[k]) for a, (i, k) in zip(accs, pairs)
            )

        return lax.fori_loop(0, span // 16, one, accs)

    accs = tuple(jnp.zeros((8, LANES), jnp.float32) for _ in pairs)
    for o in near:
        whole_copy(o, peer[o]).wait_recv()
    for c in range(CHUNKS):
        for o in far:
            gram_copy(o, c, peer[o]).wait_recv()
        accs = gram(c * span, accs)

    value = dict(zip(pairs, accs))
    for i, k in pairs:
        if i == k:
            dist[i * workers + i] = jnp.zeros((8, LANES), jnp.float32)
        else:
            d = value[i, i] + value[k, k] - 2.0 * value[i, k]
            dist[i * workers + k] = d
            dist[k * workers + i] = d
    lists.wait()
    for i in range(workers):
        s = dist[i * workers + nb_ref[0, i]]
        for j in range(1, nb_ref.shape[0]):
            s = s + dist[i * workers + nb_ref[j, i]]
        part[pl.ds(i, 1), :] = jnp.sum(s, axis=0, keepdims=True)

    def z_copy(z):
        return pltpu.make_async_remote_copy(
            src_ref=part,
            dst_ref=zbuf.at[z],
            send_sem=zsend.at[z],
            recv_sem=zrecv.at[z],
            device_id={"mp": (plane + z) % planes},
            device_id_type=MESH,
        )

    def p_copy(o):
        return pltpu.make_async_remote_copy(
            src_ref=plane_part,
            dst_ref=pbuf.at[o],
            send_sem=psend.at[o],
            recv_sem=precv.at[o],
            device_id={"worker": peer[o]},
            device_id_type=MESH,
        )

    for z in range(1, planes):
        z_copy(z).start()
    for ox in rest_order:
        if split:
            first = (ox - 1) * half
            relay_copy(ox).wait_recv()
            add_to_rest(
                flip(chip, 3 - ox, chips),
                first,
                half,
                lambda at, first=first, ox=ox: relay[
                    ox - 1, pl.ds(pl.multiple_of(at.start - first, block), block), :
                ],
            )
    for ox in rest_order:
        rest_copy(ox).start()
    total = part[...]
    for z in range(1, planes):
        z_copy(z).wait_recv()
        total = total + zbuf[z]
    plane_part[...] = total
    for o in range(1, workers):
        p_copy(o).start()

    for ox in rest_order:
        rest_copy(ox).wait_recv()

    def finish(step, carry):
        at = pl.ds(pl.multiple_of(step * block, block), block)
        low = rest_in[chip, at, :].astype(jnp.float32)
        for ox in rest_order:
            low = low + rest_recv[ox, at, :].astype(jnp.float32)
        out_ref[at, :] = recv[win_ref[0], at, :].astype(jnp.float32) + low
        return carry

    lax.fori_loop(0, rows // block, finish, 0)

    for o in range(1, workers):
        p_copy(o).wait_recv()
        total = total + pbuf[o]
    column = jnp.sum(total, axis=1, keepdims=True) / jnp.float32(total_entries)
    line = lax.broadcasted_iota(jnp.int32, (workers, LANES), 0)
    lane = lax.broadcasted_iota(jnp.int32, (workers, LANES), 1)
    scores_ref[...] = jnp.sum(
        jnp.where(line == lane, column, 0.0), axis=0, keepdims=True
    )[:, :workers]

    for ox in range(chips):
        swap(ox).wait_send()
    if split:
        relay_copy(1).wait_send()
        relay_copy(2).wait_send()
    for o in near:
        whole_copy(o, me).wait_send()
    for o in far:
        for c in range(CHUNKS):
            gram_copy(o, c, me).wait_send()
    for ox in rest_order:
        rest_copy(ox).wait_send()
    for z in range(1, planes):
        z_copy(z).wait_send()
    for o in range(1, workers):
        p_copy(o).wait_send()


def emit(scores_ref, block_ref, scores_out, block_out, sems):
    copies = [
        pltpu.make_async_copy(block_ref, block_out, sems.at[0]),
        pltpu.make_async_copy(scores_ref, scores_out, sems.at[1]),
    ]
    for copy in copies:
        copy.start()
    for copy in copies:
        copy.wait()


def solution(mesh):
    workers = mesh.shape["worker"]
    planes = mesh.shape["mp"]
    chips = workers // 2

    def body(gradients, neighbours, winner):
        length = gradients.shape[1]
        rows = length // (LANES * workers)
        entries = neighbours.shape[1] * length * planes
        bf16, f32 = jnp.bfloat16, jnp.float32
        dma = pltpu.SemaphoreType.DMA
        scores, aggregate = pl.pallas_call(
            functools.partial(kernel, workers, planes, entries),
            out_shape=(
                pltpu.VMEM((1, workers), f32),
                pltpu.VMEM((rows, LANES), f32),
            ),
            in_specs=[
                pl.BlockSpec(memory_space=pltpu.HBM),
                pl.BlockSpec(memory_space=pltpu.SMEM),
                pl.BlockSpec(memory_space=pltpu.HBM),
            ],
            out_specs=(
                pl.BlockSpec(memory_space=pltpu.VMEM),
                pl.BlockSpec(memory_space=pltpu.VMEM),
            ),
            scratch_shapes=[
                pltpu.SMEM(neighbours.shape[::-1], jnp.int32),
                pltpu.VMEM((workers, rows, LANES), f32),
                pltpu.VMEM((workers, rows, LANES), bf16),
                pltpu.VMEM((workers, rows, LANES), bf16),
                pltpu.VMEM((2, chips, rows, LANES), bf16),
                pltpu.VMEM((chips, rows, LANES), bf16),
                pltpu.VMEM((chips, rows, LANES), bf16),
                pltpu.VMEM((2, rows // 2, LANES), bf16),
                pltpu.VMEM((workers * workers, 8, LANES), f32),
                pltpu.VMEM((workers, LANES), f32),
                pltpu.VMEM((planes, workers, LANES), f32),
                pltpu.VMEM((workers, LANES), f32),
                pltpu.VMEM((workers, workers, LANES), f32),
                dma,
                dma((workers,)),
                dma((workers, CHUNKS)),
                dma((workers, CHUNKS)),
                dma((chips,)),
                dma((chips,)),
                dma((2,)),
                dma((2,)),
                dma((chips,)),
                dma((chips,)),
                dma((planes,)),
                dma((planes,)),
                dma((workers,)),
                dma((workers,)),
            ],
            compiler_params=pltpu.CompilerParams(
                collective_id=0, has_side_effects=True, vmem_limit_bytes=63_500_000
            ),
        )(neighbours.T, winner, gradients.reshape(length // LANES, LANES))
        scores, aggregate = pl.pallas_call(
            emit,
            out_shape=(
                jax.ShapeDtypeStruct(scores.shape, f32),
                jax.ShapeDtypeStruct(aggregate.shape, f32),
            ),
            in_specs=[pl.BlockSpec(memory_space=pltpu.VMEM)] * 2,
            out_specs=(pl.BlockSpec(memory_space=pl.ANY),) * 2,
            scratch_shapes=[dma((2,))],
            compiler_params=pltpu.CompilerParams(vmem_limit_bytes=8 * 1024 * 1024),
        )(scores, aggregate)
        return scores.reshape(workers), aggregate.reshape(rows * LANES)

    in_specs = (P("worker", "mp"), P(), P())
    out_specs = (P(), P(("mp", "worker")))
    return jax.shard_map(body, mesh=mesh, in_specs=in_specs, out_specs=out_specs, check_vma=False)
```
